8 devices in a mesh: data: 1 (over z), dap: 8 (over y, x, core).
Axes of the slice: x: 2, y: 2, z: 1, core: 2. Of those that a mesh axis runs over, the one named last changes fastest.
Arguments:
- pair_rep: bfloat16 [6, 640, 640, 128], P('data', 'dap')
- pair_mask: int32 [6, 640, 640], P('data', 'dap')
- norm_gain: bfloat16 [2, 128], replicated
- norm_bias: bfloat16 [2, 128], replicated
- w_proj: bfloat16 [2, 128, 512], replicated
- w_gate: bfloat16 [2, 128, 128], replicated
- hid_gain: bfloat16 [2, 128], replicated
- hid_bias: bfloat16 [2, 128], replicated
- w_out: bfloat16 [2, 128, 128], replicated
Outputs:
- output: bfloat16 [6, 640, 640, 128], P('data', None, 'dap')
All inputs are finite; a program needn't handle non-finite values.
Results may differ from the reference program's by a relative error of at most 0.00632151.
Values are sent between devices in bfloat16 or wider.
A program may use at most 1 GiB of HBM per device.

```python
import jax
import jax.numpy as jnp
from jax import lax

NUM_CROPS = 6
N_RES = 640
C_PAIR = 128
C_HIDDEN = 128
LN_EPS = 1e-5
BLOCK_ROWS = min(N_RES, 64)


def setup_inputs(seed: int = 0, part: int = 0) -> dict:
    key_list = jax.random.split(jax.random.key(seed), 8)
    part_key = jax.random.fold_in(key_list[0], part)
    key_pair, key_keep, key_len = jax.random.split(part_key, 3)
    pair_vals = jax.random.normal(key_pair, (NUM_CROPS, N_RES, N_RES, C_PAIR), jnp.float32)
    keep_res = jax.random.randint(key_keep, (NUM_CROPS, N_RES), 0, 16) != 0
    pad_len = jax.random.randint(key_len, (NUM_CROPS, 1), 0, N_RES // 8 + 1)
    res_valid = (keep_res & (jnp.arange(N_RES)[None, :] < N_RES - pad_len)).astype(jnp.int32)
    pair_mask = res_valid[:, :, None] * res_valid[:, None, :]
    norm_gain = 1.0 + 0.3 * jax.random.normal(key_list[1], (2, C_PAIR), jnp.float32)
    norm_bias = 0.3 * jax.random.normal(key_list[2], (2, C_PAIR), jnp.float32)
    w_proj = jax.random.normal(key_list[3], (2, C_PAIR, 4 * C_HIDDEN), jnp.float32) * C_PAIR ** -0.5
    w_gate = jax.random.normal(key_list[4], (2, C_PAIR, C_PAIR), jnp.float32) * C_PAIR ** -0.5
    hid_gain = 1.0 + 0.3 * jax.random.normal(key_list[5], (2, C_HIDDEN), jnp.float32)
    hid_bias = 0.3 * jax.random.normal(key_list[6], (2, C_HIDDEN), jnp.float32)
    w_out = jax.random.normal(key_list[7], (2, C_HIDDEN, C_PAIR), jnp.float32) * C_HIDDEN ** -0.5
    return {
        'pair_rep': pair_vals.astype(jnp.bfloat16),
        'pair_mask': pair_mask,
        'norm_gain': norm_gain.astype(jnp.bfloat16),
        'norm_bias': norm_bias.astype(jnp.bfloat16),
        'w_proj': w_proj.astype(jnp.bfloat16),
        'w_gate': w_gate.astype(jnp.bfloat16),
        'hid_gain': hid_gain.astype(jnp.bfloat16),
        'hid_bias': hid_bias.astype(jnp.bfloat16),
        'w_out': w_out.astype(jnp.bfloat16),
    }


def layer_norm(values, gain_vec, bias_vec):
    centred = values - jnp.mean(values, axis=-1, keepdims=True)
    var_val = jnp.mean(centred * centred, axis=-1, keepdims=True)
    return centred * lax.rsqrt(var_val + LN_EPS) * gain_vec.astype(jnp.float32) + bias_vec.astype(jnp.float32)


def project(pair_rows, mask_rows, norm_gain, norm_bias, w_proj):
    normed = layer_norm(pair_rows.astype(jnp.float32), norm_gain, norm_bias).astype(jnp.bfloat16)
    proj_all = jnp.dot(normed.reshape(-1, C_PAIR), w_proj, preferred_element_type=jnp.float32)
    proj_all = proj_all.reshape(BLOCK_ROWS, N_RES, 4, C_HIDDEN)
    mask_f = mask_rows.astype(jnp.float32)[:, :, None]
    left_proj = (mask_f * jax.nn.sigmoid(proj_all[:, :, 1]) * proj_all[:, :, 0]).astype(jnp.bfloat16)
    right_proj = (mask_f * jax.nn.sigmoid(proj_all[:, :, 3]) * proj_all[:, :, 2]).astype(jnp.bfloat16)
    return left_proj, right_proj


def finish(pair_rows, tri_sum, norm_gain, norm_bias, w_gate, hid_gain, hid_bias, w_out):
    normed = layer_norm(pair_rows.astype(jnp.float32), norm_gain, norm_bias).astype(jnp.bfloat16)
    gate_val = jax.nn.sigmoid(jnp.dot(normed.reshape(-1, C_PAIR), w_gate, preferred_element_type=jnp.float32))
    tri_round = tri_sum.astype(jnp.bfloat16).astype(jnp.float32)
    hid_norm = layer_norm(tri_round, hid_gain, hid_bias).astype(jnp.bfloat16)
    out_proj = jnp.dot(hid_norm.reshape(-1, C_HIDDEN), w_out, preferred_element_type=jnp.float32)
    new_rows = pair_rows.astype(jnp.float32) + (gate_val * out_proj).reshape(BLOCK_ROWS, N_RES, C_PAIR)
    return new_rows.astype(jnp.bfloat16)


def tri_update(pair_grid, mask_grid, weights, layer_idx, incoming):
    norm_gain, norm_bias, w_proj, w_gate, hid_gain, hid_bias, w_out = [w_arr[layer_idx] for w_arr in weights]
    n_blocks = N_RES // BLOCK_ROWS

    def proj_block(blk_idx):
        row_start = blk_idx * BLOCK_ROWS
        pair_rows = lax.dynamic_slice_in_dim(pair_grid, row_start, BLOCK_ROWS, 0)
        mask_rows = lax.dynamic_slice_in_dim(mask_grid, row_start, BLOCK_ROWS, 0)
        return project(pair_rows, mask_rows, norm_gain, norm_bias, w_proj)

    left_proj, right_proj = lax.map(proj_block, jnp.arange(n_blocks))
    left_proj = left_proj.reshape(N_RES, N_RES, C_HIDDEN)
    right_all = right_proj.reshape(N_RES, N_RES, C_HIDDEN).astype(jnp.float32)

    def out_block(blk_idx):
        row_start = blk_idx * BLOCK_ROWS
        pair_rows = lax.dynamic_slice_in_dim(pair_grid, row_start, BLOCK_ROWS, 0)
        if incoming:
            left_blk = lax.dynamic_slice_in_dim(left_proj, row_start, BLOCK_ROWS, 1).astype(jnp.float32)
            tri_sum = jnp.einsum('kic,kjc->ijc', left_blk, right_all)
        else:
            left_blk = lax.dynamic_slice_in_dim(left_proj, row_start, BLOCK_ROWS, 0).astype(jnp.float32)
            tri_sum = jnp.einsum('ikc,jkc->ijc', left_blk, right_all)
        return finish(pair_rows, tri_sum, norm_gain, norm_bias, w_gate, hid_gain, hid_bias, w_out)

    new_grid = lax.map(out_block, jnp.arange(n_blocks))
    return new_grid.reshape(N_RES, N_RES, C_PAIR)


def reference(pair_rep, pair_mask, norm_gain, norm_bias, w_proj, w_gate, hid_gain, hid_bias, w_out):
    weights = (norm_gain, norm_bias, w_proj, w_gate, hid_gain, hid_bias, w_out)

    def per_crop(crop_item):
        pair_grid, mask_grid = crop_item
        mid_grid = tri_update(pair_grid, mask_grid, weights, 0, False)
        return tri_update(mid_grid, mask_grid, weights, 1, True)

    return lax.map(per_crop, (pair_rep, pair_mask))
```

```python
import functools

import jax
import jax.numpy as jnp
from jax import lax
from jax.experimental import pallas as pl
from jax.experimental.pallas import tpu as pltpu
from jax.sharding import PartitionSpec as P

F32, BF16 = jnp.float32, jnp.bfloat16
LN_EPS = 1e-5
CH = 128
RB = 16
CB = 4
MB = 512
SUB = 8
N_DEV = 8
FIRST = {0: 0, 2: 1, 4: 2, 6: 3}
SECOND = {1: 4, 7: 5}
ORDER = (1, 2, 4, 3, 5, 6, 7)
OUT_CHUNKS = 2
NT = (((1,), (1,)), ((), ()))
TN = (((0,), (0,)), ((), ()))
VMEM_LIMIT = 62 * 1024 * 1024


def ln_lanes(vals, gain, bias):
    cen = vals - jnp.mean(vals, axis=-1, keepdims=True)
    var = jnp.mean(cen * cen, axis=-1, keepdims=True)
    return cen * lax.rsqrt(var + LN_EPS) * gain + bias


def sigm(vals):
    return 0.5 * jnp.tanh(0.5 * vals) + 0.5


def project_block(z_ref, m_ref, gain_ref, bias_ref, wt_ref, x_ref, a_ref, b_ref, sa_ref, sb_ref):
    gain = gain_ref[...]
    bias = bias_ref[...]

    def cols_body(kc, carry):
        cols = pl.ds(pl.multiple_of(kc * CH, CH), CH)
        for rp in range(RB // 2):
            z = z_ref[2 * rp:2 * rp + 2, cols, :].astype(F32).reshape(2 * CH, CH)
            x = ln_lanes(z, gain, bias).astype(BF16)
            x_ref[2 * rp:2 * rp + 2, cols, :] = x.reshape(2, CH, CH)
            q = lax.dot_general(wt_ref[...], x, NT, preferred_element_type=F32)
            for half in range(2):
                lanes = slice(half * CH, (half + 1) * CH)
                row = 2 * rp + half
                msk = m_ref[row, :, cols].astype(F32)
                dst = (row // SUB, pl.ds(row % SUB, CH, stride=SUB), slice(None))
                sa_ref[dst] = msk * sigm(q[CH:2 * CH, lanes]) * q[:CH, lanes]
                sb_ref[dst] = msk * sigm(q[3 * CH:, lanes]) * q[2 * CH:3 * CH, lanes]
        for cg in range(CH // SUB):
            at = slice(cg * SUB * SUB, (cg + 1) * SUB * SUB)
            for src, dst in ((sa_ref, a_ref), (sb_ref, b_ref)):
                parts = [src[h, at, :].reshape(SUB, SUB, CH) for h in range(RB // SUB)]
                dst[cg * SUB:(cg + 1) * SUB, :, cols] = jnp.concatenate(parts, axis=1).astype(BF16)
        return carry

    lax.fori_loop(0, z_ref.shape[1] // CH, cols_body, 0)


def finish_block(z_ref, x_ref, t_ref, hg_ref, hb_ref, wgo_ref, out_ref, st_ref, lhs_ref):
    def cols_body(kc, carry):
        cols = pl.ds(pl.multiple_of(kc * CH, CH), CH)
        for cg in range(CH // SUB):
            blk = t_ref[cg * SUB:(cg + 1) * SUB, :, cols].astype(F32)
            for h in range(RB // SUB):
                st_ref[h, cg * SUB * SUB:(cg + 1) * SUB * SUB, :] = blk[:, SUB * h:SUB * h + SUB, :].reshape(SUB * SUB, CH)
        for r in range(RB):
            t = st_ref[r // SUB, pl.ds(r % SUB, CH, stride=SUB), :]
            cen = t - jnp.mean(t, axis=0, keepdims=True)
            var = jnp.mean(cen * cen, axis=0, keepdims=True)
            hid = (cen * lax.rsqrt(var + LN_EPS) * hg_ref[...] + hb_ref[...]).astype(BF16)
            lhs_ref[r * CH:(r + 1) * CH, :CH] = x_ref[r, cols, :]
            lhs_ref[r * CH:(r + 1) * CH, CH:] = hid.T
        nr = MB // CH
        for g in range(RB // nr):
            go = jnp.dot(lhs_ref[g * MB:(g + 1) * MB, :], wgo_ref[...], preferred_element_type=F32)
            z = z_ref[g * nr:(g + 1) * nr, cols, :].astype(F32).reshape(MB, CH)
            new = (z + sigm(go[:, :CH]) * go[:, CH:]).astype(BF16)
            out_ref[g * nr:(g + 1) * nr, cols, :] = new.reshape(nr, CH, CH)
        return carry

    lax.fori_loop(0, z_ref.shape[1] // CH, cols_body, 0)


def proj_kernel(n_alias, s_ref, z_ref, m_ref, gain_ref, bias_ref, wt_ref, *refs):
    zo_ref, x_ref, a_ref, b_ref, sa_ref, sb_ref = refs[n_alias:]

    @pl.when(s_ref[0] == 1)
    def _():
        zo_ref[...] = z_ref[...]
        project_block(z_ref, m_ref, gain_ref, bias_ref, wt_ref, x_ref, a_ref, b_ref, sa_ref, sb_ref)


def full_spec(arr):
    return pl.BlockSpec(arr.shape, lambda i, s: (0,) * arr.ndim)


def params():
    return pltpu.CompilerParams(vmem_limit_bytes=VMEM_LIMIT)


def project(on, row0, piece, mask, wts, bufs):
    rows, width, _ = piece.shape
    gain, bias, wt = wts
    n_alias = len(bufs)
    pos_spec = pl.BlockSpec((RB, width, CH), lambda i, s: (s[1] + i * s[0], 0, 0))
    chan_spec = pl.BlockSpec((CH, RB, width), lambda i, s: (0, s[1] + i * s[0], 0))
    pos = jax.ShapeDtypeStruct((width, width, CH), BF16)
    chan = jax.ShapeDtypeStruct((CH, width, width), BF16)
    return pl.pallas_call(
        functools.partial(proj_kernel, n_alias),
        grid_spec=pltpu.PrefetchScalarGridSpec(
            num_scalar_prefetch=1, grid=(rows // RB,),
            in_specs=[
                pl.BlockSpec((RB, width, CH), lambda i, s: (i * s[0], 0, 0)),
                pl.BlockSpec((RB, 1, width), lambda i, s: (s[1] + i * s[0], 0, 0)),
                full_spec(gain), full_spec(bias), full_spec(wt),
            ] + [pl.BlockSpec(memory_space=pl.ANY)] * n_alias,
            out_specs=[pos_spec, pos_spec, chan_spec, chan_spec],
            scratch_shapes=[pltpu.VMEM((RB // SUB, CH * SUB, CH), F32)] * 2,
        ),
        out_shape=[pos, pos, chan, chan],
        input_output_aliases={6 + i: i for i in range(n_alias)},
        compiler_params=params(),
        cost_estimate=pl.CostEstimate(flops=2 * rows * width * 8 * CH * CH, bytes_accessed=12 * rows * width * CH, transcendentals=0),
        name="project",
    )(jnp.stack([on, row0]), piece, mask, gain, bias, wt, *bufs)


def tri_kernel(dims, s_ref, a_ref, b_ref, t_ref):
    @pl.when(s_ref[0] == 1)
    def _():
        for c in range(CB):
            t_ref[c] = lax.dot_general(a_ref[c], b_ref[c], dims, preferred_element_type=F32).astype(BF16)


def triangle(on, a, b, incoming):
    chans, size, _ = a.shape
    spec = pl.BlockSpec((CB, size, size), lambda c, s: (c * s[0], 0, 0))
    return pl.pallas_call(
        functools.partial(tri_kernel, TN if incoming else NT),
        grid_spec=pltpu.PrefetchScalarGridSpec(
            num_scalar_prefetch=1, grid=(chans // CB,), in_specs=[spec, spec], out_specs=spec),
        out_shape=jax.ShapeDtypeStruct(a.shape, BF16),
        input_output_aliases={1: 0},
        compiler_params=params(),
        cost_estimate=pl.CostEstimate(flops=2 * chans * size ** 3, bytes_accessed=6 * chans * size * size, transcendentals=0),
        name="tri_in" if incoming else "tri_out",
    )(jnp.full((1,), on, jnp.int32), a, b)


def mid_kernel(s_ref, z_ref, x_ref, t_ref, m_ref, hg_ref, hb_ref, wgo_ref, gain_ref, bias_ref, wt_ref,
               zo_ref, xo_ref, a_ref, b_ref, st_ref, lhs_ref, sb_ref):
    @pl.when(s_ref[0] == 1)
    def _():
        finish_block(z_ref, x_ref, t_ref, hg_ref, hb_ref, wgo_ref, zo_ref, st_ref, lhs_ref)
        project_block(zo_ref, m_ref, gain_ref, bias_ref, wt_ref, xo_ref, a_ref, b_ref, st_ref, sb_ref)


def middle(on, z, x, t, mask, fin, wts):
    size = z.shape[0]
    pos_spec = pl.BlockSpec((RB, size, CH), lambda i, s: (i * s[0], 0, 0))
    chan_spec = pl.BlockSpec((CH, RB, size), lambda i, s: (0, i * s[0], 0))
    pos = jax.ShapeDtypeStruct(z.shape, BF16)
    chan = jax.ShapeDtypeStruct(t.shape, BF16)
    swap = pltpu.VMEM((RB // SUB, CH * SUB, CH), F32)
    return pl.pallas_call(
        mid_kernel,
        grid_spec=pltpu.PrefetchScalarGridSpec(
            num_scalar_prefetch=1, grid=(size // RB,),
            in_specs=[pos_spec, pos_spec, chan_spec, pl.BlockSpec((RB, 1, size), lambda i, s: (i * s[0], 0, 0))]
            + [full_spec(w) for w in (*fin, *wts)],
            out_specs=[pos_spec, pos_spec, chan_spec, chan_spec],
            scratch_shapes=[swap, pltpu.VMEM((RB * CH, 2 * CH), BF16), swap],
        ),
        out_shape=[pos, pos, chan, chan],
        input_output_aliases={1: 0, 2: 1, 3: 2},
        compiler_params=params(),
        cost_estimate=pl.CostEstimate(flops=2 * size * size * 12 * CH * CH, bytes_accessed=14 * size * size * CH, transcendentals=0),
        name="middle",
    )(jnp.full((1,), on, jnp.int32), z, x, t, mask, *fin, *wts)


def last_kernel(s_ref, z_ref, x_ref, t_ref, hg_ref, hb_ref, wgo_ref, *refs):
    outs, (res_ref, st_ref, lhs_ref) = refs[:N_DEV], refs[N_DEV:]
    part = outs[0].shape[1]

    @pl.when(s_ref[0] == 1)
    def _():
        finish_block(z_ref, x_ref, t_ref, hg_ref, hb_ref, wgo_ref, res_ref, st_ref, lhs_ref)
        for s in range(N_DEV):
            first = pl.multiple_of(jnp.bitwise_xor(s_ref[1], s) * part, 16)
            outs[s][...] = res_ref[:, pl.ds(first, part), :]


def last(on, me, chunk, z, x, t, fin):
    size = z.shape[0]
    rows = size // OUT_CHUNKS
    blk0 = chunk * (rows // RB)
    part = size // N_DEV
    pos_spec = pl.BlockSpec((RB, size, CH), lambda i, s: (blk0 + i * s[0], 0, 0))
    return pl.pallas_call(
        last_kernel,
        grid_spec=pltpu.PrefetchScalarGridSpec(
            num_scalar_prefetch=1, grid=(rows // RB,),
            in_specs=[pos_spec, pos_spec, pl.BlockSpec((CH, RB, size), lambda i, s: (0, blk0 + i * s[0], 0))]
            + [full_spec(w) for w in fin],
            out_specs=[pl.BlockSpec((RB, part, CH), lambda i, s: (i * s[0], 0, 0))] * N_DEV,
            scratch_shapes=[pltpu.VMEM((RB, size, CH), BF16), pltpu.VMEM((RB // SUB, CH * SUB, CH), F32),
                            pltpu.VMEM((RB * CH, 2 * CH), BF16)],
        ),
        out_shape=[jax.ShapeDtypeStruct((rows, part, CH), BF16)] * N_DEV,
        compiler_params=params(),
        cost_estimate=pl.CostEstimate(flops=2 * rows * size * 4 * CH * CH, bytes_accessed=8 * rows * size * CH, transcendentals=0),
        name="last",
    )(jnp.stack([on, me]), z, x, t, *fin)


PLACE_ROWS = 160


def place_kernel(n_in, s_ref, *refs):
    out_ref = refs[-1]
    for s in range(n_in):
        @pl.when(s_ref[0] == s)
        def _():
            out_ref[0] = refs[s][...]


def place(sel, crop, chunk, pieces, out, out_shape):
    rows, part, _ = pieces[0].shape
    steps = rows // PLACE_ROWS

    def in_spec(s):
        return pl.BlockSpec((PLACE_ROWS, part, CH), lambda i, sr: (jnp.where(sr[0] == s, i, 0), 0, 0))

    bufs = [] if out is None else [out]
    return pl.pallas_call(
        functools.partial(place_kernel, N_DEV),
        grid_spec=pltpu.PrefetchScalarGridSpec(
            num_scalar_prefetch=1, grid=(steps,),
            in_specs=[in_spec(s) for s in range(N_DEV)] + [pl.BlockSpec(memory_space=pl.ANY)] * len(bufs),
            out_specs=pl.BlockSpec((1, PLACE_ROWS, part, CH), lambda i, sr: (crop, chunk * steps + i, 0, 0)),
        ),
        out_shape=jax.ShapeDtypeStruct(out_shape, BF16),
        input_output_aliases={1 + N_DEV: 0} if bufs else {},
        compiler_params=params(),
        name="place",
    )(jnp.full((1,), sel, jnp.int32), *pieces, *bufs)


def lookup(table, index, missing):
    val = jnp.int32(missing)
    for key, entry in table.items():
        val = jnp.where(index == key, entry, val)
    return val


def tie(vals, *others):
    return lax.optimization_barrier((tuple(vals), tuple(others)))[0]


def solution(mesh):
    def shard_body(pair_stack, mask_stack, norm_gain, norm_bias, w_proj, w_gate, hid_gain, hid_bias, w_out):
        me = lax.axis_index("dap")
        n_crops, rows, size, _ = pair_stack.shape
        pad = jnp.zeros((CH, CH), BF16)
        fins, projs = [], []
        for u in range(2):
            wgo = jnp.block([[w_gate[u], pad], [pad, w_out[u]]])
            spread = lambda v: jnp.broadcast_to(v.astype(F32)[:, None], (CH, CH))
            fins.append((spread(hid_gain[u]), spread(hid_bias[u]), wgo))
            projs.append((norm_gain[u].astype(F32)[None], norm_bias[u].astype(F32)[None], w_proj[u].T))

        owner_crop = {**FIRST, **SECOND}
        mask_sends = jnp.stack([mask_stack[owner_crop.get(d, 0)] for d in range(N_DEV)]).astype(BF16)
        mask = lax.all_to_all(mask_sends, "dap", 0, 0, tiled=True).reshape(size, 1, size)

        def gather(owners, after):
            pieces = {}
            source = tie((pair_stack,), *after)[0] if after else pair_stack
            for s in (*ORDER, 0):
                crop = lookup(owners, jnp.bitwise_xor(me, s), 0)
                pieces[s] = lax.dynamic_index_in_dim(source, crop, 0, keepdims=False)
                source = tie((source,), pieces[s])[0]
            for s in ORDER:
                pieces[s] = lax.ppermute(pieces[s], "dap", [(d ^ s, d) for d in owners])
            return pieces

        def update(on, pieces):
            bufs = ()
            for s in (0, *ORDER):
                row0 = jnp.bitwise_xor(me, s) * (rows // RB)
                bufs = project(on, row0, pieces[s], mask, projs[0], bufs)
            z, x, a, b = bufs
            z, x, a, b = middle(on, z, x, triangle(on, a, b, False), mask, fins[0], projs[1])
            t = triangle(on, a, b, True)
            return [last(on, me, k, z, x, t, fins[1]) for k in range(OUT_CHUNKS)]

        def hand_out(owners, sends):
            return [[arr if s == 0 else lax.ppermute(arr, "dap", [(d, d ^ s) for d in owners])
                     for s, arr in enumerate(chunk)] for chunk in sends]

        on_first = lookup({d: 1 for d in FIRST}, me, 0)
        on_second = lookup({d: 1 for d in SECOND}, me, 0)
        first = gather(FIRST, ())
        second = gather(SECOND, [first[s] for s in ORDER])
        sends_first = update(on_first, first)
        got_first = hand_out(FIRST, sends_first)
        second = {s: tie((arr,), *[c[0] for c in sends_first])[0] for s, arr in second.items()}
        sends_second = update(on_second, second)
        got_second = hand_out(SECOND, sends_second)
        out = None
        for owners, got in ((FIRST, got_first), (SECOND, got_second)):
            for k in range(OUT_CHUNKS):
                for dev, crop in owners.items():
                    out = place(jnp.bitwise_xor(me, dev), crop, k, got[k], out, (n_crops, size, rows, CH))
        return out

    rep = P()
    in_specs = (P("data", "dap", None, None), P("data", "dap", None)) + (rep,) * 7
    return jax.shard_map(shard_body, mesh=mesh, in_specs=in_specs,
                         out_specs=P("data", None, "dap", None), check_vma=False)
```

```python
import functools

import jax
import jax.numpy as jnp
from jax import lax
from jax.experimental import pallas as pl
from jax.experimental.pallas import tpu as pltpu
from jax.sharding import PartitionSpec as P


F32, BF16 = jnp.float32, jnp.bfloat16
LN_EPS = 1e-5
CH = 128
RB = 16
CB = 4
MB = 512
SUB = 8
N_DEV = 8
FIRST = {0: 0, 2: 1, 4: 2, 6: 3}
SECOND = {1: 4, 7: 5}
ORDER = (1, 2, 4, 3, 5, 6, 7)
USE_SECOND = (1, 2, 3, 4, 5, 6, 7)
OUT_CHUNKS = 2
NT = (((1,), (1,)), ((), ()))
TN = (((0,), (0,)), ((), ()))
VMEM_LIMIT = 62 * 1024 * 1024


def ln_lanes(vals, gain, bias):
    cen = vals - jnp.mean(vals, axis=-1, keepdims=True)
    var = jnp.mean(cen * cen, axis=-1, keepdims=True)
    return cen * lax.rsqrt(var + LN_EPS) * gain + bias


def gated(half_gate, half_val):
    return (jnp.tanh(half_gate) + 1.0) * half_val


def project_block(z_ref, m_ref, gain_ref, bias_ref, wt_ref, x_ref, a_ref, b_ref, sa_ref, sb_ref):
    gain = gain_ref[...]
    bias = bias_ref[...]

    def cols_body(kc, carry):
        cols = pl.ds(pl.multiple_of(kc * CH, CH), CH)
        for rp in range(RB // 2):
            z = z_ref[2 * rp:2 * rp + 2, cols, :].astype(F32).reshape(2 * CH, CH)
            x = ln_lanes(z, gain, bias).astype(BF16)
            x_ref[2 * rp:2 * rp + 2, cols, :] = x.reshape(2, CH, CH)
            q = lax.dot_general(wt_ref[...], x, NT, preferred_element_type=F32)
            for half in range(2):
                lanes = slice(half * CH, (half + 1) * CH)
                row = 2 * rp + half
                msk = m_ref[row, :, cols].astype(F32)
                dst = (row // SUB, pl.ds(row % SUB, CH, stride=SUB), slice(None))
                sa_ref[dst] = msk * gated(q[CH:2 * CH, lanes], q[:CH, lanes])
                sb_ref[dst] = msk * gated(q[3 * CH:, lanes], q[2 * CH:3 * CH, lanes])
        for cg in range(CH // SUB):
            at = slice(cg * SUB * SUB, (cg + 1) * SUB * SUB)
            for src, dst in ((sa_ref, a_ref), (sb_ref, b_ref)):
                parts = [src[h, at, :].reshape(SUB, SUB, CH) for h in range(RB // SUB)]
                dst[cg * SUB:(cg + 1) * SUB, :, cols] = jnp.concatenate(parts, axis=1).astype(BF16)
        return carry

    lax.fori_loop(0, z_ref.shape[1] // CH, cols_body, 0)


def finish_block(z_ref, x_ref, t_ref, hg_ref, hb_ref, wgo_ref, out_ref, st_ref, lhs_ref):
    def cols_body(kc, carry):
        cols = pl.ds(pl.multiple_of(kc * CH, CH), CH)
        for cg in range(CH // SUB):
            blk = t_ref[cg * SUB:(cg + 1) * SUB, :, cols].astype(F32)
            for h in range(RB // SUB):
                st_ref[h, cg * SUB * SUB:(cg + 1) * SUB * SUB, :] = blk[:, SUB * h:SUB * h + SUB, :].reshape(SUB * SUB, CH)
        for r in range(RB):
            t = st_ref[r // SUB, pl.ds(r % SUB, CH, stride=SUB), :]
            cen = t - jnp.mean(t, axis=0, keepdims=True)
            var = jnp.mean(cen * cen, axis=0, keepdims=True)
            hid = (cen * lax.rsqrt(var + LN_EPS) * hg_ref[...] + hb_ref[...]).astype(BF16)
            lhs_ref[r * CH:(r + 1) * CH, :CH] = x_ref[r, cols, :]
            lhs_ref[r * CH:(r + 1) * CH, CH:] = hid.T
        nr = MB // CH
        for g in range(RB // nr):
            go = jnp.dot(lhs_ref[g * MB:(g + 1) * MB, :], wgo_ref[...], preferred_element_type=F32)
            z = z_ref[g * nr:(g + 1) * nr, cols, :].astype(F32).reshape(MB, CH)
            new = (z + gated(go[:, :CH], go[:, CH:])).astype(BF16)
            out_ref[g * nr:(g + 1) * nr, cols, :] = new.reshape(nr, CH, CH)
        return carry

    lax.fori_loop(0, z_ref.shape[1] // CH, cols_body, 0)


def proj_kernel(n_alias, s_ref, z_ref, m_ref, gain_ref, bias_ref, wt_ref, *refs):
    zo_ref, x_ref, a_ref, b_ref, sa_ref, sb_ref = refs[n_alias:]

    @pl.when(s_ref[0] == 1)
    def _():
        zo_ref[...] = z_ref[...]
        project_block(z_ref, m_ref, gain_ref, bias_ref, wt_ref, x_ref, a_ref, b_ref, sa_ref, sb_ref)


def full_spec(arr):
    return pl.BlockSpec(arr.shape, lambda i, s: (0,) * arr.ndim)


def params():
    return pltpu.CompilerParams(vmem_limit_bytes=VMEM_LIMIT)


def project(on, row0, piece, mask, wts, bufs):
    rows, width, _ = piece.shape
    gain, bias, wt = wts
    n_alias = len(bufs)
    pos_spec = pl.BlockSpec((RB, width, CH), lambda i, s: (s[1] + i * s[0], 0, 0))
    chan_spec = pl.BlockSpec((CH, RB, width), lambda i, s: (0, s[1] + i * s[0], 0))
    pos = jax.ShapeDtypeStruct((width, width, CH), BF16)
    chan = jax.ShapeDtypeStruct((CH, width, width), BF16)
    return pl.pallas_call(
        functools.partial(proj_kernel, n_alias),
        grid_spec=pltpu.PrefetchScalarGridSpec(
            num_scalar_prefetch=1, grid=(rows // RB,),
            in_specs=[
                pl.BlockSpec((RB, width, CH), lambda i, s: (i * s[0], 0, 0)),
                pl.BlockSpec((RB, 1, width), lambda i, s: (s[1] + i * s[0], 0, 0)),
                full_spec(gain), full_spec(bias), full_spec(wt),
            ] + [pl.BlockSpec(memory_space=pl.ANY)] * n_alias,
            out_specs=[pos_spec, pos_spec, chan_spec, chan_spec],
            scratch_shapes=[pltpu.VMEM((RB // SUB, CH * SUB, CH), F32)] * 2,
        ),
        out_shape=[pos, pos, chan, chan],
        input_output_aliases={6 + i: i for i in range(n_alias)},
        compiler_params=params(),
        cost_estimate=pl.CostEstimate(flops=2 * rows * width * 8 * CH * CH, bytes_accessed=12 * rows * width * CH, transcendentals=0),
        name="project",
    )(jnp.stack([on, row0]), piece, mask, gain, bias, wt, *bufs)


def tri_kernel(dims, s_ref, a_ref, b_ref, t_ref):
    @pl.when(s_ref[0] == 1)
    def _():
        for c in range(CB):
            t_ref[c] = lax.dot_general(a_ref[c], b_ref[c], dims, preferred_element_type=F32).astype(BF16)


def triangle(on, a, b, incoming):
    chans, size, _ = a.shape
    spec = pl.BlockSpec((CB, size, size), lambda c, s: (c * s[0], 0, 0))
    return pl.pallas_call(
        functools.partial(tri_kernel, TN if incoming else NT),
        grid_spec=pltpu.PrefetchScalarGridSpec(
            num_scalar_prefetch=1, grid=(chans // CB,), in_specs=[spec, spec], out_specs=spec),
        out_shape=jax.ShapeDtypeStruct(a.shape, BF16),
        input_output_aliases={1: 0},
        compiler_params=params(),
        cost_estimate=pl.CostEstimate(flops=2 * chans * size ** 3, bytes_accessed=6 * chans * size * size, transcendentals=0),
        name="tri_in" if incoming else "tri_out",
    )(jnp.full((1,), on, jnp.int32), a, b)


def mid_kernel(s_ref, z_ref, x_ref, t_ref, m_ref, hg_ref, hb_ref, wgo_ref, gain_ref, bias_ref, wt_ref,
               zo_ref, xo_ref, a_ref, b_ref, st_ref, lhs_ref, sb_ref):
    @pl.when(s_ref[0] == 1)
    def _():
        finish_block(z_ref, x_ref, t_ref, hg_ref, hb_ref, wgo_ref, zo_ref, st_ref, lhs_ref)
        project_block(zo_ref, m_ref, gain_ref, bias_ref, wt_ref, xo_ref, a_ref, b_ref, st_ref, sb_ref)


def middle(on, z, x, t, mask, fin, wts):
    size = z.shape[0]
    pos_spec = pl.BlockSpec((RB, size, CH), lambda i, s: (i * s[0], 0, 0))
    chan_spec = pl.BlockSpec((CH, RB, size), lambda i, s: (0, i * s[0], 0))
    pos = jax.ShapeDtypeStruct(z.shape, BF16)
    chan = jax.ShapeDtypeStruct(t.shape, BF16)
    swap = pltpu.VMEM((RB // SUB, CH * SUB, CH), F32)
    return pl.pallas_call(
        mid_kernel,
        grid_spec=pltpu.PrefetchScalarGridSpec(
            num_scalar_prefetch=1, grid=(size // RB,),
            in_specs=[pos_spec, pos_spec, chan_spec, pl.BlockSpec((RB, 1, size), lambda i, s: (i * s[0], 0, 0))]
            + [full_spec(w) for w in (*fin, *wts)],
            out_specs=[pos_spec, pos_spec, chan_spec, chan_spec],
            scratch_shapes=[swap, pltpu.VMEM((RB * CH, 2 * CH), BF16), swap],
        ),
        out_shape=[pos, pos, chan, chan],
        input_output_aliases={1: 0, 2: 1, 3: 2},
        compiler_params=params(),
        cost_estimate=pl.CostEstimate(flops=2 * size * size * 12 * CH * CH, bytes_accessed=14 * size * size * CH, transcendentals=0),
        name="middle",
    )(jnp.full((1,), on, jnp.int32), z, x, t, mask, *fin, *wts)


def last_kernel(s_ref, z_ref, x_ref, t_ref, hg_ref, hb_ref, wgo_ref, *refs):
    outs, (res_ref, st_ref, lhs_ref) = refs[:N_DEV], refs[N_DEV:]
    part = outs[0].shape[1]

    @pl.when(s_ref[0] == 1)
    def _():
        finish_block(z_ref, x_ref, t_ref, hg_ref, hb_ref, wgo_ref, res_ref, st_ref, lhs_ref)
        for s in range(N_DEV):
            first = pl.multiple_of(jnp.bitwise_xor(s_ref[1], s) * part, 16)
            outs[s][...] = res_ref[:, pl.ds(first, part), :]


def last(on, me, chunk, z, x, t, fin):
    size = z.shape[0]
    rows = size // OUT_CHUNKS
    blk0 = chunk * (rows // RB)
    part = size // N_DEV
    pos_spec = pl.BlockSpec((RB, size, CH), lambda i, s: (blk0 + i * s[0], 0, 0))
    return pl.pallas_call(
        last_kernel,
        grid_spec=pltpu.PrefetchScalarGridSpec(
            num_scalar_prefetch=1, grid=(rows // RB,),
            in_specs=[pos_spec, pos_spec, pl.BlockSpec((CH, RB, size), lambda i, s: (0, blk0 + i * s[0], 0))]
            + [full_spec(w) for w in fin],
            out_specs=[pl.BlockSpec((RB, part, CH), lambda i, s: (i * s[0], 0, 0))] * N_DEV,
            scratch_shapes=[pltpu.VMEM((RB, size, CH), BF16), pltpu.VMEM((RB // SUB, CH * SUB, CH), F32),
                            pltpu.VMEM((RB * CH, 2 * CH), BF16)],
        ),
        out_shape=[jax.ShapeDtypeStruct((rows, part, CH), BF16)] * N_DEV,
        compiler_params=params(),
        cost_estimate=pl.CostEstimate(flops=2 * rows * size * 4 * CH * CH, bytes_accessed=8 * rows * size * CH, transcendentals=0),
        name="last",
    )(jnp.stack([on, me]), z, x, t, *fin)


PLACE_ROWS = 160


def place_kernel(n_in, s_ref, *refs):
    out_ref = refs[-1]
    for s in range(n_in):
        @pl.when(s_ref[0] == s)
        def _():
            out_ref[0] = refs[s][...]


def place(sel, crop, chunk, pieces, out, out_shape):
    rows, part, _ = pieces[0].shape
    steps = rows // PLACE_ROWS

    def in_spec(s):
        return pl.BlockSpec((PLACE_ROWS, part, CH), lambda i, sr: (jnp.where(sr[0] == s, i, 0), 0, 0))

    bufs = [] if out is None else [out]
    return pl.pallas_call(
        functools.partial(place_kernel, N_DEV),
        grid_spec=pltpu.PrefetchScalarGridSpec(
            num_scalar_prefetch=1, grid=(steps,),
            in_specs=[in_spec(s) for s in range(N_DEV)] + [pl.BlockSpec(memory_space=pl.ANY)] * len(bufs),
            out_specs=pl.BlockSpec((1, PLACE_ROWS, part, CH), lambda i, sr: (crop, chunk * steps + i, 0, 0)),
        ),
        out_shape=jax.ShapeDtypeStruct(out_shape, BF16),
        input_output_aliases={1 + N_DEV: 0} if bufs else {},
        compiler_params=params(),
        name="place",
    )(jnp.full((1,), sel, jnp.int32), *pieces, *bufs)


def lookup(table, index, missing):
    val = jnp.int32(missing)
    for key, entry in table.items():
        val = jnp.where(index == key, entry, val)
    return val


def tie(vals, *others):
    return lax.optimization_barrier((tuple(vals), tuple(others)))[0]


def solution(mesh):
    def shard_body(pair_stack, mask_stack, norm_gain, norm_bias, w_proj, w_gate, hid_gain, hid_bias, w_out):
        me = lax.axis_index("dap")
        n_crops, rows, size, _ = pair_stack.shape
        pad = jnp.zeros((CH, CH), BF16)
        half = jnp.asarray(0.5, BF16)
        fins, projs = [], []
        for u in range(2):
            wgo = jnp.block([[w_gate[u], pad], [pad, w_out[u]]]) * half
            spread = lambda v: jnp.broadcast_to(v.astype(F32)[:, None], (CH, CH))
            fins.append((spread(hid_gain[u]), spread(hid_bias[u]), wgo))
            projs.append((norm_gain[u].astype(F32)[None], norm_bias[u].astype(F32)[None], w_proj[u].T * half))

        owner_crop = {**FIRST, **SECOND}
        mask_sends = jnp.stack([mask_stack[owner_crop.get(d, 0)] for d in range(N_DEV)]).astype(BF16)
        mask = lax.all_to_all(mask_sends, "dap", 0, 0, tiled=True)
        mask = mask.reshape(size, 1, size)

        def cut(owners, source):
            cuts = {}
            for s in (*ORDER, 0):
                crop = lookup(owners, jnp.bitwise_xor(me, s), 0)
                cuts[s] = lax.dynamic_index_in_dim(source, crop, 0, keepdims=False)
                source = tie((source,), cuts[s])[0]
            return cuts, source

        def gather(owners, cuts):
            pieces = {0: cuts[0]}
            for s in ORDER:
                pieces[s] = lax.ppermute(cuts[s], "dap", [(d ^ s, d) for d in owners])
            return pieces

        def update(on, pieces, order):
            bufs = ()
            for s in (0, *order):
                row0 = jnp.bitwise_xor(me, s) * (rows // RB)
                bufs = project(on, row0, pieces[s], mask, projs[0], bufs)
            z, x, a, b = bufs
            z, x, a, b = middle(on, z, x, triangle(on, a, b, False), mask, fins[0], projs[1])
            t = triangle(on, a, b, True)
            return [last(on, me, k, z, x, t, fins[1]) for k in range(OUT_CHUNKS)]

        def hand_out(owners, sends):
            return [[arr if s == 0 else lax.ppermute(arr, "dap", [(d, d ^ s) for d in owners])
                     for s, arr in enumerate(chunk)] for chunk in sends]

        on_first = lookup({d: 1 for d in FIRST}, me, 0)
        on_second = lookup({d: 1 for d in SECOND}, me, 0)
        cuts_first, source = cut(FIRST, pair_stack)
        cuts_second, _ = cut(SECOND, source)
        first = gather(FIRST, cuts_first)
        cuts_second = dict(zip(cuts_second, tie(cuts_second.values(), *[first[s] for s in ORDER])))
        second = gather(SECOND, cuts_second)
        sends_first = update(on_first, first, ORDER)
        got_first = hand_out(FIRST, sends_first)
        second = {s: tie((arr,), *[c[0] for c in sends_first])[0] for s, arr in second.items()}
        sends_second = update(on_second, second, USE_SECOND)
        got_second = hand_out(SECOND, sends_second)
        out = None
        for owners, got in ((FIRST, got_first), (SECOND, got_second)):
            for k in range(OUT_CHUNKS):
                for dev, crop in owners.items():
                    out = place(jnp.bitwise_xor(me, dev), crop, k, got[k], out, (n_crops, size, rows, CH))
        return out

    rep = P()
    in_specs = (P("data", "dap", None, None), P("data", "dap", None)) + (rep,) * 7

    return jax.shard_map(shard_body, mesh=mesh, in_specs=in_specs,
                         out_specs=P("data", None, "dap", None), check_vma=False)
```
